32 devices in a mesh: blk: 16 (over z, y, core), tgt: 2 (over x).
Axes of the slice: x: 2, y: 2, z: 4, core: 2. Of those that a mesh axis runs over, the one named last changes fastest.
Arguments:
- history: float32 [32768, 1536], P(('blk', 'tgt')), may hold values from 0 to 2
- weights: bfloat16 [16, 2048, 32768], P(None, 'tgt', 'blk'), may hold values from -0.03125 to 0.03125
- delays: int32 [8, 8], replicated, may hold values from 16 to 64
- area_blocks: int32 [8], replicated, may hold values from 1 to 3, 16 in all
- potential: float32 [24, 32768], P(None, ('blk', 'tgt')), may hold values from -6 to 6
- leak: float32 [32768], P(('blk', 'tgt')), may hold values from 0.03 to 0.6
- drive: float32 [32768], P(('blk', 'tgt')), may hold values from -6 to 6
Outputs:
- rate_steps: float32 [16, 24, 32768], P(None, None, ('blk', 'tgt'))
- last_potential: float32 [24, 32768], P(None, ('blk', 'tgt'))
The draws below stay inside these ranges and needn't reach their ends.
Inputs may be any that keep to these rules, and one draw needn't show every extreme that they name: Area a consists of area_blocks[a] consecutive blocks of 2048 neurons; areas follow one another in order.
All inputs are finite; a program needn't handle non-finite values.
Results may differ from the reference program's by a relative error of at most 0.00083.
Values may be sent and summed in bfloat16 or wider, within the bound.
No kernel may reach another device: no remote copies, remote signals or barrier semaphores. Data moves between devices by JAX's collectives and lax.ppermute only.
A program may use at most 192 MiB of HBM per device.

```python
import math
import jax
import jax.numpy as jnp
import numpy as np
from jax import lax

NEURONS = 32768
TRIAL_TOTAL = 24
STEPS = 16
HIST = 64
AREAS = 8
BLOCK = 2048
N_BLK = 16


def place_ends(values, own_key, smallest, largest):
    extent = values.shape
    index_at = [jax.random.randint(jax.random.fold_in(own_key, axis), (), 0, extent[axis]) for axis in range(len(extent))]
    values = values.at[tuple(index_at)].set(smallest)
    longest = extent.index(max(extent))
    index_at[longest] = (index_at[longest] + 1) % extent[longest]
    return values.at[tuple(index_at)].set(largest)


def block_levels(key, shape, split, low, largest):
    factor_of = 1.0
    for axis_at, parts in split:
        draws = jax.random.uniform(jax.random.fold_in(jax.random.fold_in(key, 6), axis_at), (parts,), jnp.float32, low / len(split), largest / len(split))
        factor_of = factor_of * jnp.repeat(jnp.exp(draws), shape[axis_at] // parts).reshape((-1,) + (1,) * (len(shape) - 1 - axis_at))
    return factor_of


def length_profile(count, total, bound, skew):
    portions = [(1 << 20) // math.isqrt(rank ** skew) + 1 for rank in range(2, count + 1)]
    rest, counts = total - bound - (count - 1), [1] * (count - 1)
    while rest > 0:
        candidates = [i for i in range(count - 1) if counts[i] < bound]
        mass, left = sum([portions[i] for i in candidates]), rest
        for i in candidates:
            addition = min(bound - counts[i], max(1, left * portions[i] // mass), rest)
            counts[i] = counts[i] + addition
            rest = rest - addition
    return np.array([bound] + counts)


def ragged_sizes(key, number_of, total, limit, slope):
    if number_of == 2:
        one = jax.random.randint(key, (), max(1, total - limit), min(limit, total - 1) + 1)
        return jnp.stack([one, total - one])
    lengths = jnp.asarray(length_profile(number_of, total, limit, slope), jnp.int32)
    twos = (number_of - 1) // 2
    source_of, receiver = lengths[1:1 + 2 * twos:2], lengths[2:2 + 2 * twos:2]
    slack = jnp.minimum(source_of - 1, limit - receiver)
    moved = jax.random.randint(jax.random.fold_in(key, 1), (twos,), 0, 1 << 20) % (slack + 1)
    lengths = lengths.at[1:1 + 2 * twos:2].set(source_of - moved).at[2:2 + 2 * twos:2].set(receiver + moved)
    return lengths[jax.random.permutation(jax.random.fold_in(key, 2), number_of)]


def scatter_about(stream_key, extent, spread, limit, split=(), held_as=jnp.bfloat16):
    array = spread * jax.random.normal(stream_key, extent, jnp.float32)
    if split:
        array = array * block_levels(stream_key, extent, split, -0.22, 0.18)
    return jnp.clip(array, -limit, limit).astype(held_as)


def setup_inputs(seed: int = 0) -> dict:
    key_list = jax.random.split(jax.random.key(seed), 8)
    return {
        "history": jnp.clip(2.0 * jax.random.uniform(key_list[0], (NEURONS, HIST * TRIAL_TOTAL), jnp.float32) ** block_levels(key_list[0], (NEURONS, HIST * TRIAL_TOTAL), ((0, 32),), -0.2, 0.2), 0.0, 2.0),
        "weights": scatter_about(key_list[1], (N_BLK, BLOCK, NEURONS), NEURONS ** -0.5, 0.03125, ((1, 2), (2, 16))),
        "delays": place_ends(jax.random.randint(key_list[2], (AREAS, AREAS), 16, 65), jax.random.fold_in(key_list[2], 1), 16, 64).astype(jnp.int32),
        "area_blocks": ragged_sizes(key_list[3], AREAS, N_BLK, 3, 1).astype(jnp.int32),
        "potential": scatter_about(key_list[4], (TRIAL_TOTAL, NEURONS), 1.0, 6.0, ((1, 32),), jnp.float32),
        "leak": jnp.clip(jnp.exp(math.log(0.6) - 2.9957323 * jax.random.uniform(key_list[5], (NEURONS,), jnp.float32) ** block_levels(key_list[5], (NEURONS,), ((0, 32),), -0.2, 0.2)), 0.03, 0.6),
        "drive": scatter_about(key_list[6], (NEURONS,), 1.0, 6.0, ((0, 32),), jnp.float32),
    }


def block_areas(area_blocks, block_count):
    boundary = jnp.cumsum(area_blocks)
    blocks = jnp.arange(block_count, dtype=jnp.int32)
    return jnp.sum((boundary[None, :] <= blocks[:, None]).astype(jnp.int32), axis=1)


def reference(history, weights, delays, area_blocks, potential, leak, drive):
    area_of_block = block_areas(area_blocks, N_BLK)
    history_low = history.astype(jnp.bfloat16).reshape(N_BLK, BLOCK, HIST * TRIAL_TOTAL)

    def window(lag_step, column):
        start = ((HIST - lag_step) * TRIAL_TOTAL).astype(jnp.int32)
        return lax.dynamic_slice_in_dim(column, start, STEPS * TRIAL_TOTAL, 1)

    def one_target(target_block):
        lag_steps = delays[area_of_block[target_block]][area_of_block]
        delayed_input = jax.vmap(window, in_axes=(0, 0))(lag_steps, history_low)
        weight_column_slice = lax.dynamic_slice_in_dim(weights, (target_block * BLOCK).astype(jnp.int32), BLOCK, 2)
        return jnp.einsum("gyw,gyt->wt", delayed_input.astype(jnp.float32), weight_column_slice.astype(jnp.float32))

    inputs = lax.map(one_target, jnp.arange(N_BLK, dtype=jnp.int32))
    inputs = inputs.transpose(1, 0, 2).reshape(STEPS, TRIAL_TOTAL, NEURONS)

    def advance(membrane_state, synaptic):
        membrane_state = membrane_state + leak * (drive - membrane_state + synaptic)
        return membrane_state, jax.nn.softplus(membrane_state)

    last_potential, rate_steps = lax.scan(advance, potential, inputs)
    return rate_steps, last_potential
```

```python
import functools
import jax
import jax.numpy as jnp
from jax import lax
from jax.experimental import pallas as pl
from jax.experimental.pallas import tpu as pltpu
from jax.sharding import PartitionSpec as P

STEPS = 16
CHUNKS = 2
GROUP = 4
FORCE = None
SUB = 8


def turn(history, chunks):
    rows, columns = history.shape
    width = rows // chunks
    tile = 384 if columns % 384 == 0 else columns

    def kernel(x_ref, *out_refs):
        for k, out_ref in enumerate(out_refs):
            out_ref[...] = x_ref[k * width : (k + 1) * width, :].T.astype(jnp.bfloat16)

    return pl.pallas_call(
        kernel,
        grid=(columns // tile,),
        in_specs=[pl.BlockSpec((rows, tile), lambda i: (0, i))],
        out_specs=[pl.BlockSpec((tile, width), lambda i: (i, 0))] * chunks,
        out_shape=[jax.ShapeDtypeStruct((columns, width), jnp.bfloat16)] * chunks,
        name="turn",
    )(history)


def gain(starts, arrived, weights, chunk, depth, shares, total=None, split=None):
    blocks, _, _, width = arrived.shape
    targets = weights.shape[2]
    share = targets // shares
    length = depth // SUB
    given = total is not None

    def kernel(start_ref, *refs):
        old_ref = refs[0] if given else None
        a_ref, w_ref, *out_refs = refs[1 if given else 0 : -1]
        sum_ref = refs[-1]
        i = pl.program_id(0)
        product = jnp.dot(a_ref[0].reshape(depth, width), w_ref[0], preferred_element_type=jnp.float32)

        @pl.when(i == 0)
        def _():
            sum_ref[...] = product + old_ref[...] if given else product

        @pl.when(i > 0)
        def _():
            sum_ref[...] += product

        @pl.when(i == blocks - 1)
        def _():
            if split is None:
                out_refs[0][...] = sum_ref[...]
            else:
                for k in range(shares):
                    for out_ref in out_refs:
                        out_ref[k] = sum_ref[:, k * share : (k + 1) * share].astype(out_ref.dtype)

    whole = pl.BlockSpec((depth, targets), lambda i, s: (0, 0))
    if split is None:
        outs = [jax.ShapeDtypeStruct((depth, targets), jnp.float32)]
        out_specs = [whole]
    else:
        outs = [jax.ShapeDtypeStruct((shares, depth, share), t) for t in split]
        out_specs = [pl.BlockSpec((shares, depth, share), lambda i, s: (0, 0, 0))] * len(split)
    return pl.pallas_call(
        kernel,
        grid_spec=pltpu.PrefetchScalarGridSpec(
            num_scalar_prefetch=1,
            grid=(blocks,),
            in_specs=([whole] if given else [])
            + [
                pl.BlockSpec(
                    (pl.Element(1), pl.Element(length), pl.Element(SUB), pl.Element(width)),
                    lambda i, s: (i, s[i], 0, 0),
                ),
                pl.BlockSpec((1, width, targets), lambda i, s: (i, chunk, 0)),
            ],
            out_specs=out_specs,
            scratch_shapes=[pltpu.VMEM((depth, targets), jnp.float32)],
        ),
        out_shape=outs,
        cost_estimate=pl.CostEstimate(
            flops=2 * depth * width * blocks * targets,
            bytes_accessed=2 * width * blocks * (targets + depth),
            transcendentals=0,
        ),
        name="gain",
    )(starts, *([total] if given else []), arrived, weights)


def advance(share_at, own, arrived, potential, leak, drive):
    trials, share = potential.shape
    steps = own[0].shape[1]

    def kernel(at_ref, *refs):
        own_refs, in_refs = refs[: len(own)], refs[len(own) : len(own) + len(arrived)]
        potential_ref, leak_ref, drive_ref, rate_ref, last_ref = refs[-5:]
        membrane = potential_ref[...]
        leak_row, drive_row = leak_ref[...], drive_ref[...]
        for s in range(steps):
            synaptic = own_refs[0][0, s]
            for ref in own_refs[1:]:
                synaptic += ref[0, s]
            for ref in in_refs:
                synaptic += ref[s].astype(jnp.float32)
            membrane = membrane + leak_row * (drive_row - membrane + synaptic)
            rate_ref[s] = jnp.maximum(membrane, 0.0) + jnp.log1p(jnp.exp(-jnp.abs(membrane)))
        last_ref[...] = membrane

    tile = 256 if share % 256 == 0 else share
    wide = pl.BlockSpec((steps, trials, tile), lambda i, a: (0, 0, i))
    flat = pl.BlockSpec((trials, tile), lambda i, a: (0, i))
    line = pl.BlockSpec((1, tile), lambda i, a: (0, i))
    mine = pl.BlockSpec((1, steps, trials, tile), lambda i, a: (a[0], 0, 0, i))
    return pl.pallas_call(
        kernel,
        grid_spec=pltpu.PrefetchScalarGridSpec(
            num_scalar_prefetch=1,
            grid=(share // tile,),
            in_specs=[mine] * len(own) + [wide] * len(arrived) + [flat, line, line],
            out_specs=[wide, flat],
        ),
        out_shape=[
            jax.ShapeDtypeStruct((steps, trials, share), jnp.float32),
            jax.ShapeDtypeStruct(potential.shape, jnp.float32),
        ],
        name="advance",
    )(share_at[None], *own, *arrived, potential, leak[None], drive[None])


def collect(table, inputs, sizes, cases, length, chosen=None):
    width = inputs[0].shape[2]

    def kernel(table_ref, *refs):
        in_refs, out_refs, sems = refs[: len(inputs)], refs[len(inputs) : -1], refs[-1]

        def carry_out(case):
            copies = [
                pltpu.make_async_copy(
                    in_refs[a].at[pl.ds(table_ref[entry], length)],
                    out_refs[o].at[pl.ds(place * length, length)],
                    sems.at[n],
                )
                for n, (a, entry, o, place) in enumerate(case)
            ]
            for copy in copies:
                copy.start()
            for copy in copies:
                copy.wait()

        if chosen is None:
            carry_out(cases[0])
        else:
            for n, case in enumerate(cases):
                pl.when(table_ref[chosen] == n)(functools.partial(carry_out, case))

    outs = [jax.ShapeDtypeStruct((n * length, SUB, width), jnp.bfloat16) for n in sizes]
    return pl.pallas_call(
        kernel,
        grid_spec=pltpu.PrefetchScalarGridSpec(
            num_scalar_prefetch=1,
            grid=(1,),
            in_specs=[pl.BlockSpec(memory_space=pltpu.MemorySpace.HBM)] * len(inputs),
            out_specs=[pl.BlockSpec(o.shape, lambda i, t: (0, 0, 0)) for o in outs],
            scratch_shapes=[pltpu.SemaphoreType.DMA((max(len(c) for c in cases),))],
        ),
        out_shape=outs,
        cost_estimate=pl.CostEstimate(flops=3 * 10**9, bytes_accessed=6 << 20, transcendentals=0),
        name="collect",
    )(table, *inputs)


def gain_group(table, entry, windows, weights, halves, depth, shares, total=None, part=None, kind=jnp.float32):
    width = windows[0].shape[2]
    targets = weights.shape[2]
    share = targets // shares
    tile = 512 if share % 512 == 0 else share
    tiles = share // tile
    length = depth // SUB
    given = total is not None

    def kernel(table_ref, *refs):
        old_ref = refs[0] if given else None
        refs = refs[1 if given else 0 :]
        a_refs, w_refs, out_ref = refs[:GROUP], refs[GROUP:-1], refs[-1]
        value = old_ref[0] if given else None
        for n in range(len(halves)):
            for j in range(GROUP):
                a = a_refs[j][n * length : (n + 1) * length].reshape(depth, width)
                product = jnp.dot(a, w_refs[n * GROUP + j][0], preferred_element_type=jnp.float32)
                value = product if value is None else value + product
        out_ref[0] = value.astype(out_ref.dtype)

    def share_of(i, t):
        return i // tiles if part is None else lax.rem(t[AT_SHARE] + part, shares)

    def weight_at(half, j):
        return lambda i, t: (t[entry + j], half, share_of(i, t) * tiles + i % tiles)

    parts = shares if part is None else 1
    return pl.pallas_call(
        kernel,
        grid_spec=pltpu.PrefetchScalarGridSpec(
            num_scalar_prefetch=1,
            grid=(parts * tiles,),
            in_specs=([pl.BlockSpec((1, depth, tile), lambda i, t: (share_of(i, t), 0, i % tiles))] if given else [])
            + [pl.BlockSpec(w.shape, lambda i, t: (0, 0, 0)) for w in windows]
            + [pl.BlockSpec((1, width, tile), weight_at(h, j)) for h in halves for j in range(GROUP)],
            out_specs=pl.BlockSpec((1, depth, tile), lambda i, t: (i // tiles, 0, i % tiles)),
        ),
        out_shape=jax.ShapeDtypeStruct((parts, depth, share), kind),
        cost_estimate=pl.CostEstimate(
            flops=2 * depth * width * len(halves) * GROUP * parts * share, bytes_accessed=16 << 20, transcendentals=0
        ),
        name="gain_group",
    )(table, *([total] if given else []), *windows, *([weights] * (GROUP * len(halves))))


LINE = 4
ORDER = ((1, 2, 3), (0, 2, 3), (3, 1, 0), (2, 1, 0))
CASE = ((3, 3, 3), (0, 1, 1), (1, 0, 0), (2, 2, 2))
FORWARDS = ((0, 1), (0, -1), (1, 1), (1, -1), (2, 1), (2, -1))


def at_window(o, j):
    return o * GROUP + j


def at_slot(f, k):
    return LINE * GROUP + f * GROUP + k


AT_CASE = LINE * GROUP + len(FORWARDS) * GROUP
AT_BLOCK = AT_CASE + LINE
AT_SHARE = AT_BLOCK + LINE * GROUP
AT_COUNT = AT_SHARE + 1
ENTRIES = AT_COUNT + 1


def plan(area_blocks, delays, place, hist, per):
    areas = area_blocks.shape[0]
    blocks = LINE * GROUP
    length = STEPS * per

    def kernel(sizes_ref, delays_ref, place_ref, out_ref, area_ref):
        for b in range(blocks):
            edge, area = jnp.int32(0), jnp.int32(0)
            for a in range(areas):
                edge = edge + sizes_ref[a]
                area = area + (edge <= b).astype(jnp.int32)
            area_ref[b] = jnp.minimum(area, areas - 1)
        group, member = place_ref[0], place_ref[1]

        def of_group(values):
            picked = jnp.int32(values[0])
            for g in range(1, LINE):
                picked = jnp.where(group == g, values[g], picked)
            return picked

        def start(target_area, source_group):
            return (hist - delays_ref[target_area, area_ref[source_group * GROUP + member]]) * per

        mine = area_ref[group * GROUP]
        for o in range(LINE):
            source = group if o == 0 else of_group([r[o - 1] for r in ORDER])
            case = jnp.int32(0) if o == 0 else of_group([r[o - 1] for r in CASE])
            out_ref[AT_CASE + o] = case
            for j in range(GROUP):
                peer = area_ref[group * GROUP + (member ^ j)]
                out_ref[at_window(o, j)] = jnp.where(case >= 2, (peer - mine) * length, start(peer, source))
                out_ref[AT_BLOCK + o * GROUP + j] = source * GROUP + (member ^ j)
        for f, (made, d) in enumerate(FORWARDS):
            beyond = jnp.clip(group + d, 0, LINE - 1) * GROUP
            source = jnp.clip(group - made * d, 0, LINE - 1)
            for k in range(GROUP):
                area = jnp.minimum(area_ref[beyond] + k, area_ref[beyond + GROUP - 1])
                out_ref[at_slot(f, k)] = start(area, source)
        out_ref[AT_SHARE] = place_ref[2]
        outer = [area_ref[g * GROUP + GROUP - 1] - area_ref[g * GROUP] for g in (0, LINE - 1)]
        out_ref[AT_COUNT] = jnp.maximum(outer[0], outer[1])

    smem = pl.BlockSpec(memory_space=pltpu.MemorySpace.SMEM)
    return pl.pallas_call(
        kernel,
        in_specs=[smem] * 3,
        out_specs=smem,
        out_shape=jax.ShapeDtypeStruct((ENTRIES,), jnp.int32),
        scratch_shapes=[pltpu.SMEM((blocks,), jnp.int32)],
        name="plan",
    )(area_blocks, delays, place)


def line_of_groups(slot_count, table, turned, weights, potential, leak, drive, *, size, shares):
    targets = weights.shape[2]
    trials = potential.shape[0]
    per = trials // SUB
    length = STEPS * per
    depth = STEPS * trials
    share = targets // shares
    last = LINE - 1

    def hop(x, s, d, outer):
        pairs = []
        for g in range(LINE):
            to = g + d
            if 0 <= to <= last and 0 <= to - s * d <= last and (to == (last if d == 1 else 0)) == outer:
                pairs += [(g * GROUP + m, to * GROUP + m) for m in range(GROUP)]
        return lax.ppermute(x, "blk", pairs)

    def swap(windows):
        given = [windows[0]]
        for j in range(1, GROUP):
            given.append(lax.ppermute(windows[j], "blk", [(b, b ^ j) for b in range(size)]))
        return given

    def tie(later, earlier):
        return lax.optimization_barrier((later, earlier))[0]

    ab = range(2)
    counts = [slot_count] * 2
    full, slots = {}, {}
    last_step = []

    def gather(inputs, sizes, cases, chosen=None):
        inputs = tie(inputs, last_step) if last_step else inputs
        outs = collect(table, inputs, sizes, cases, length, chosen)
        last_step[:] = outs
        return outs

    def forward(s, h):
        if s == 2:
            for d in (1, -1):
                full[s, d, h] = hop(full[s - 1, d, h], s, d, False)
        outs = gather(
            [full[s - 1, 1, h], full[s - 1, -1, h]], counts,
            [[(f, at_slot(2 * (s - 1) + f, k), f, k) for f in ab for k in range(slot_count)]],
        )
        for f, d in enumerate((1, -1)):
            slots[s, d, h] = hop(outs[f], s, d, True)

    def windows_of(o, halves):
        inner = {1: (1, 1), 2: (1, 1), 3: (2, 2)}[o]
        buffers = [full[inner[0], 1, h] for h in halves] + [full[inner[1], -1, h] for h in halves]
        buffers += [slots[o, 1, h] for h in halves] + [slots[o, -1, h] for h in halves]
        n = len(halves)
        cases = [
            [(c * n + h, at_window(o, j), j, h) for j in range(GROUP) for h in range(n)] for c in range(4)
        ]
        return swap(gather(buffers, [n] * GROUP, cases, AT_CASE + o))

    def add(o, windows, halves, total=None, part=None, kind=jnp.float32):
        windows = [tie(windows[0], last_step)] + windows[1:]
        return gain_group(
            table, AT_BLOCK + o * GROUP, windows, weights, halves, depth, shares, total, part, kind
        )

    share_at = table[AT_SHARE]
    shape = (STEPS, trials, share)
    came = []

    def send(part, k):
        came.append(lax.ppermute(part, "tgt", [(t, (t + k) % shares) for t in range(shares)]).reshape(shape))

    outs = gather(
        turned, counts * 2, [[(h, at_slot(f, k), 2 * h + f, k) for h in ab for f in ab for k in range(slot_count)]]
    )
    for h in ab:
        for f, d in enumerate((1, -1)):
            slots[1, d, h] = hop(outs[2 * h + f], 1, d, True)
            full[1, d, h] = hop(turned[h], 1, d, False)
    own = gather(turned, [2] * GROUP, [[(h, at_window(0, j), j, h) for j in range(GROUP) for h in ab]])
    own = swap(own)
    forward(2, 0)
    first = windows_of(1, ab)
    forward(2, 1)
    total = add(0, own, ab)
    forward(3, 0)
    second = windows_of(2, ab)
    early = add(1, first, ab, total)
    for k in range(1, shares):
        send(lax.dynamic_index_in_dim(early, (share_at + k) % shares, 0, False), k)
    forward(3, 1)
    third = [windows_of(3, (0,))]
    third += [windows_of(3, (1,))]
    late = add(2, second, ab)
    late = add(3, third[0], (0,), late)
    for k in range(1, shares):
        send(add(3, third[1], (1,), late, k, jnp.bfloat16), k)
    late = add(3, third[1], (1,), late, 0)
    return advance(
        share_at, [early.reshape((shares,) + shape)], came + [late.reshape(shape)], potential, leak, drive
    )


def gather_all(history, weights, delays, boundary, potential, leak, drive, *, size, shares, spread):
    block_count, piece, targets = weights.shape
    trials = potential.shape[0]
    hist = history.shape[1] // trials
    per = trials // SUB
    depth = STEPS * trials
    chunks = max(1, min(CHUNKS, piece // 128))
    width = piece // chunks
    share = targets // shares
    blocks = jnp.arange(block_count, dtype=jnp.int32)
    area = jnp.sum((boundary[None, :] <= blocks[:, None]).astype(jnp.int32), axis=1)
    my_area = area[lax.axis_index("blk")]
    share_at = lax.axis_index("tgt")
    starts = ((hist - delays[my_area][area]) * per).astype(jnp.int32)

    turned = turn(history, chunks)
    arrived = [
        lax.all_gather(t, "blk", axis=0, tiled=False).reshape(size, hist * per, SUB, width) for t in turned
    ]
    own, came, total = [], [], None
    for c in range(chunks):
        if c < chunks - 2:
            (total,) = gain(starts, arrived[c], weights, c, depth, shares, total)
        elif c == chunks - 2:
            (early,) = gain(starts, arrived[c], weights, c, depth, shares, total, (jnp.float32,))
            own.append(early.reshape(shares, STEPS, trials, share))
            came += spread(early)
        else:
            late, late_low = gain(
                starts, arrived[c], weights, c, depth, shares, None, (jnp.float32, jnp.bfloat16 if chunks > 1 else jnp.float32)
            )
            own.append(late.reshape(shares, STEPS, trials, share))
            came += spread(late_low)
    return advance(share_at, own, came, potential, leak, drive)


def on_device(history, weights, delays, area_blocks, potential, leak, drive, *, size, shares):
    _, piece, targets = weights.shape
    trials = potential.shape[0]
    share = targets // shares
    boundary = jnp.cumsum(area_blocks)
    share_at = lax.axis_index("tgt")

    def spread(sums):
        came = []
        for k in range(1, shares):
            part = lax.dynamic_index_in_dim(sums, (share_at + k) % shares, 0, False)
            part = lax.ppermute(part, "tgt", [(t, (t + k) % shares) for t in range(shares)])
            came.append(part.reshape(STEPS, trials, share))
        return came

    if size != LINE * GROUP or piece % 256:
        return tuple(
            gather_all(history, weights, delays, boundary, potential, leak, drive, size=size, shares=shares, spread=spread)
        )
    me = lax.axis_index("blk")
    per = trials // SUB
    place = jnp.stack([me // GROUP, me % GROUP, share_at])
    table = plan(area_blocks, delays, place, history.shape[1] // trials, per)
    history = lax.optimization_barrier((history, table))[0]
    turned = [t.reshape(-1, SUB, piece // 2) for t in turn(history, 2)]
    line = functools.partial(line_of_groups, size=size, shares=shares)
    rest = (table, turned, weights, potential, leak, drive)
    if FORCE is not None:
        return tuple(line(FORCE, *rest))

    def branch(count):
        def run(*rest):
            return line(count, *rest)

        return run

    branches = [branch(count) for count in range(3, GROUP + 1)]
    return tuple(lax.switch(jnp.clip(table[AT_COUNT] - 2, 0, GROUP - 3), branches, *rest))


def solution(mesh):
    in_specs = (
        P(("blk", "tgt"), None),
        P(None, "tgt", "blk"),
        P(),
        P(),
        P(None, ("blk", "tgt")),
        P(("blk", "tgt")),
        P(("blk", "tgt")),
    )
    out_specs = (P(None, None, ("blk", "tgt")), P(None, ("blk", "tgt")))
    return jax.shard_map(
        functools.partial(on_device, size=mesh.shape["blk"], shares=mesh.shape["tgt"]),
        mesh=mesh, in_specs=in_specs, out_specs=out_specs, check_vma=False,
    )
```

```python
import functools
import jax
import jax.numpy as jnp
from jax import lax
from jax.experimental import pallas as pl
from jax.experimental.pallas import tpu as pltpu
from jax.sharding import PartitionSpec as P

STEPS = 16
CHUNKS = 2
GROUP = 4
FORCE = None
SUB = 8


def turn(history, widths):
    rows, columns = history.shape
    tile = 384 if columns % 384 == 0 else columns

    def kernel(x_ref, *out_refs):
        row = 0
        for width, out_ref in zip(widths, out_refs):
            out_ref[...] = x_ref[row : row + width, :].T.astype(jnp.bfloat16)
            row += width

    return pl.pallas_call(
        kernel,
        grid=(columns // tile,),
        in_specs=[pl.BlockSpec((rows, tile), lambda i: (0, i))],
        out_specs=[pl.BlockSpec((tile, width), lambda i: (i, 0)) for width in widths],
        out_shape=[jax.ShapeDtypeStruct((columns, width), jnp.bfloat16) for width in widths],
        name="turn",
    )(history)


def gain(starts, arrived, weights, chunk, depth, shares, total=None, split=None):
    blocks, _, _, width = arrived.shape
    targets = weights.shape[2]
    share = targets // shares
    length = depth // SUB
    given = total is not None

    def kernel(start_ref, *refs):
        old_ref = refs[0] if given else None
        a_ref, w_ref, *out_refs = refs[1 if given else 0 : -1]
        sum_ref = refs[-1]
        i = pl.program_id(0)
        product = jnp.dot(a_ref[0].reshape(depth, width), w_ref[0], preferred_element_type=jnp.float32)

        @pl.when(i == 0)
        def _():
            sum_ref[...] = product + old_ref[...] if given else product

        @pl.when(i > 0)
        def _():
            sum_ref[...] += product

        @pl.when(i == blocks - 1)
        def _():
            if split is None:
                out_refs[0][...] = sum_ref[...]
            else:
                for k in range(shares):
                    for out_ref in out_refs:
                        out_ref[k] = sum_ref[:, k * share : (k + 1) * share].astype(out_ref.dtype)

    whole = pl.BlockSpec((depth, targets), lambda i, s: (0, 0))
    if split is None:
        outs = [jax.ShapeDtypeStruct((depth, targets), jnp.float32)]
        out_specs = [whole]
    else:
        outs = [jax.ShapeDtypeStruct((shares, depth, share), t) for t in split]
        out_specs = [pl.BlockSpec((shares, depth, share), lambda i, s: (0, 0, 0))] * len(split)
    return pl.pallas_call(
        kernel,
        grid_spec=pltpu.PrefetchScalarGridSpec(
            num_scalar_prefetch=1,
            grid=(blocks,),
            in_specs=([whole] if given else [])
            + [
                pl.BlockSpec(
                    (pl.Element(1), pl.Element(length), pl.Element(SUB), pl.Element(width)),
                    lambda i, s: (i, s[i], 0, 0),
                ),
                pl.BlockSpec((1, width, targets), lambda i, s: (i, chunk, 0)),
            ],
            out_specs=out_specs,
            scratch_shapes=[pltpu.VMEM((depth, targets), jnp.float32)],
        ),
        out_shape=outs,
        cost_estimate=pl.CostEstimate(
            flops=2 * depth * width * blocks * targets,
            bytes_accessed=2 * width * blocks * (targets + depth),
            transcendentals=0,
        ),
        name="gain",
    )(starts, *([total] if given else []), arrived, weights)


def advance(share_at, own, arrived, potential, leak, drive):
    trials, share = potential.shape
    steps = STEPS

    def kernel(at_ref, *refs):
        own_refs, in_refs = refs[: len(own)], refs[len(own) : len(own) + len(arrived)]
        potential_ref, leak_ref, drive_ref, rate_ref, last_ref = refs[-5:]
        membrane = potential_ref[...]
        leak_row, drive_row = leak_ref[...], drive_ref[...]
        for s in range(steps):
            terms = [ref[0, s] for ref in own_refs] + [ref[s].astype(jnp.float32) for ref in in_refs]
            synaptic = sum(terms[1:], terms[0])
            membrane = membrane + leak_row * (drive_row - membrane + synaptic)
            rate_ref[s] = jnp.maximum(membrane, 0.0) + jnp.log1p(jnp.exp(-jnp.abs(membrane)))
        last_ref[...] = membrane

    tile = 256 if share % 256 == 0 else share
    wide = pl.BlockSpec((steps, trials, tile), lambda i, a: (0, 0, i))
    flat = pl.BlockSpec((trials, tile), lambda i, a: (0, i))
    line = pl.BlockSpec((1, tile), lambda i, a: (0, i))
    mine = pl.BlockSpec((1, steps, trials, tile), lambda i, a: (a[0], 0, 0, i))
    return pl.pallas_call(
        kernel,
        grid_spec=pltpu.PrefetchScalarGridSpec(
            num_scalar_prefetch=1,
            grid=(share // tile,),
            in_specs=[mine] * len(own) + [wide] * len(arrived) + [flat, line, line],
            out_specs=[wide, flat],
        ),
        out_shape=[
            jax.ShapeDtypeStruct((steps, trials, share), jnp.float32),
            jax.ShapeDtypeStruct(potential.shape, jnp.float32),
        ],
        name="advance",
    )(share_at[None], *own, *arrived, potential, leak[None], drive[None])


def collect(table, inputs, outputs, cases, length, chosen=None):
    def kernel(table_ref, *refs):
        in_refs, out_refs, sems = refs[: len(inputs)], refs[len(inputs) : -1], refs[-1]

        def carry_out(case):
            copies = []
            for n, (a, entry, o, place, lane) in enumerate(case):
                to = out_refs[o].at[pl.ds(place * length, length)]
                width = in_refs[a].shape[2]
                if width != out_refs[o].shape[2]:
                    to = out_refs[o].at[pl.ds(place * length, length), :, pl.ds(lane, width)]
                copies.append(
                    pltpu.make_async_copy(in_refs[a].at[pl.ds(table_ref[entry], length)], to, sems.at[n])
                )
            for copy in copies:
                copy.start()
            for copy in copies:
                copy.wait()

        if chosen is None:
            carry_out(cases[0])
        else:
            for n, case in enumerate(cases):
                pl.when(table_ref[chosen] == n)(functools.partial(carry_out, case))

    outs = [jax.ShapeDtypeStruct((n * length, SUB, width), jnp.bfloat16) for n, width in outputs]
    return pl.pallas_call(
        kernel,
        grid_spec=pltpu.PrefetchScalarGridSpec(
            num_scalar_prefetch=1,
            grid=(1,),
            in_specs=[pl.BlockSpec(memory_space=pltpu.MemorySpace.HBM)] * len(inputs),
            out_specs=[pl.BlockSpec(o.shape, lambda i, t: (0, 0, 0)) for o in outs],
            scratch_shapes=[pltpu.SemaphoreType.DMA((max(len(c) for c in cases),))],
        ),
        out_shape=outs,
        cost_estimate=pl.CostEstimate(flops=3 * 10**9, bytes_accessed=6 << 20, transcendentals=0),
        name="collect",
    )(table, *inputs)


def gain_group(table, entry, windows, weights, first_row, depth, shares, total=None, part=None, kind=jnp.float32):
    width = windows[0].shape[2]
    targets = weights.shape[2]
    share = targets // shares
    tile = 512 if share % 512 == 0 else share
    tiles = share // tile
    given = total is not None

    def kernel(table_ref, *refs):
        old_ref = refs[0] if given else None
        refs = refs[1 if given else 0 :]
        a_refs, w_refs, out_ref = refs[:GROUP], refs[GROUP:-1], refs[-1]
        value = old_ref[0] if given else None
        for a_ref, w_ref in zip(a_refs, w_refs):
            product = jnp.dot(a_ref[...].reshape(depth, width), w_ref[0], preferred_element_type=jnp.float32)
            value = product if value is None else value + product
        out_ref[0] = value.astype(out_ref.dtype)

    def share_of(i, t):
        return i // tiles if part is None else lax.rem(t[AT_SHARE] + part, shares)

    def place_of(i, t):
        return share_of(i, t) if total.shape[0] == shares else 0

    def weight_spec(j):
        def column(i, t):
            return share_of(i, t) * tiles + i % tiles

        if first_row % width == 0:
            return pl.BlockSpec((1, width, tile), lambda i, t: (t[entry + j], first_row // width, column(i, t)))
        return pl.BlockSpec(
            (pl.Element(1), pl.Element(width), pl.Element(tile)),
            lambda i, t: (t[entry + j], first_row, pl.multiple_of(column(i, t) * tile, tile)),
        )

    parts = shares if part is None else 1
    return pl.pallas_call(
        kernel,
        grid_spec=pltpu.PrefetchScalarGridSpec(
            num_scalar_prefetch=1,
            grid=(parts * tiles,),
            in_specs=([pl.BlockSpec((1, depth, tile), lambda i, t: (place_of(i, t), 0, i % tiles))] if given else [])
            + [pl.BlockSpec(w.shape, lambda i, t: (0, 0, 0)) for w in windows]
            + [weight_spec(j) for j in range(GROUP)],
            out_specs=pl.BlockSpec((1, depth, tile), lambda i, t: (i // tiles, 0, i % tiles)),
        ),
        out_shape=jax.ShapeDtypeStruct((parts, depth, share), kind),
        cost_estimate=pl.CostEstimate(
            flops=2 * depth * width * GROUP * parts * share, bytes_accessed=16 << 20, transcendentals=0
        ),
        name="gain_group",
    )(table, *([total] if given else []), *windows, *([weights] * GROUP))


LINE = 4
ORDER = ((1, 2, 3), (0, 2, 3), (3, 1, 0), (2, 1, 0))
CASE = ((3, 3, 3), (0, 1, 1), (1, 0, 0), (2, 2, 2))
FORWARDS = ((0, 1), (0, -1), (1, 1), (1, -1), (2, 1), (2, -1))


def at_window(o, j):
    return o * GROUP + j


def at_slot(f, k):
    return LINE * GROUP + f * GROUP + k


AT_CASE = LINE * GROUP + len(FORWARDS) * GROUP
AT_BLOCK = AT_CASE + LINE
AT_SHARE = AT_BLOCK + LINE * GROUP
AT_COUNT = AT_SHARE + 1
ENTRIES = AT_COUNT + 1


def plan(area_blocks, delays, place, hist, per):
    areas = area_blocks.shape[0]
    blocks = LINE * GROUP
    length = STEPS * per

    def kernel(sizes_ref, delays_ref, place_ref, out_ref, area_ref):
        for b in range(blocks):
            edge, area = jnp.int32(0), jnp.int32(0)
            for a in range(areas):
                edge = edge + sizes_ref[a]
                area = area + (edge <= b).astype(jnp.int32)
            area_ref[b] = jnp.minimum(area, areas - 1)
        group, member = place_ref[0], place_ref[1]

        def of_group(values):
            picked = jnp.int32(values[0])
            for g in range(1, LINE):
                picked = jnp.where(group == g, values[g], picked)
            return picked

        def start(target_area, source_group):
            return (hist - delays_ref[target_area, area_ref[source_group * GROUP + member]]) * per

        mine = area_ref[group * GROUP]
        for o in range(LINE):
            source = group if o == 0 else of_group([r[o - 1] for r in ORDER])
            case = jnp.int32(0) if o == 0 else of_group([r[o - 1] for r in CASE])
            out_ref[AT_CASE + o] = case
            for j in range(GROUP):
                peer = area_ref[group * GROUP + (member ^ j)]
                out_ref[at_window(o, j)] = jnp.where(case >= 2, (peer - mine) * length, start(peer, source))
                out_ref[AT_BLOCK + o * GROUP + j] = source * GROUP + (member ^ j)
        for f, (made, d) in enumerate(FORWARDS):
            beyond = jnp.clip(group + d, 0, LINE - 1) * GROUP
            source = jnp.clip(group - made * d, 0, LINE - 1)
            for k in range(GROUP):
                area = jnp.minimum(area_ref[beyond] + k, area_ref[beyond + GROUP - 1])
                out_ref[at_slot(f, k)] = start(area, source)
        out_ref[AT_SHARE] = place_ref[2]
        outer = [area_ref[g * GROUP + GROUP - 1] - area_ref[g * GROUP] for g in (0, LINE - 1)]
        out_ref[AT_COUNT] = jnp.maximum(outer[0], outer[1])

    smem = pl.BlockSpec(memory_space=pltpu.MemorySpace.SMEM)
    return pl.pallas_call(
        kernel,
        in_specs=[smem] * 3,
        out_specs=smem,
        out_shape=jax.ShapeDtypeStruct((ENTRIES,), jnp.int32),
        scratch_shapes=[pltpu.SMEM((blocks,), jnp.int32)],
        name="plan",
    )(area_blocks, delays, place)


def line_of_groups(slot_count, table, turned, weights, potential, leak, drive, *, size, shares):
    targets = weights.shape[2]
    trials = potential.shape[0]
    per = trials // SUB
    length = STEPS * per
    depth = STEPS * trials
    share = targets // shares
    last = LINE - 1

    def hop(x, s, d, outer):
        pairs = []
        for g in range(LINE):
            to = g + d
            if 0 <= to <= last and 0 <= to - s * d <= last and (to == (last if d == 1 else 0)) == outer:
                pairs += [(g * GROUP + m, to * GROUP + m) for m in range(GROUP)]
        return lax.ppermute(x, "blk", pairs)

    def swap(windows):
        given = [windows[0]]
        for j in range(1, GROUP):
            given.append(lax.ppermute(windows[j], "blk", [(b, b ^ j) for b in range(size)]))
        return given

    def tie(later, earlier):
        return lax.optimization_barrier((later, earlier))[0]

    ab = range(2)
    widths = [t.shape[2] for t in turned]
    piece = sum(widths)
    full, slots = {}, {}
    last_step = []

    def gather(inputs, outputs, cases, chosen=None):
        inputs = tie(inputs, last_step) if last_step else inputs
        outs = collect(table, inputs, outputs, cases, length, chosen)
        last_step[:] = outs
        return outs

    def forward(s, h):
        if s == 2:
            for d in (1, -1):
                full[s, d, h] = hop(full[s - 1, d, h], s, d, False)
        outs = gather(
            [full[s - 1, 1, h], full[s - 1, -1, h]], [(slot_count, widths[h])] * 2,
            [[(f, at_slot(2 * (s - 1) + f, k), f, k, 0) for f in ab for k in range(slot_count)]],
        )
        for f, d in enumerate((1, -1)):
            slots[s, d, h] = hop(outs[f], s, d, True)

    def windows_of(o, halves):
        inner = {1: (1, 1), 2: (1, 1), 3: (2, 2)}[o]
        buffers = [full[inner[0], 1, h] for h in halves] + [full[inner[1], -1, h] for h in halves]
        buffers += [slots[o, 1, h] for h in halves] + [slots[o, -1, h] for h in halves]
        n = len(halves)
        cases = [
            [(c * n + h, at_window(o, j), j, 0, h * widths[0]) for j in range(GROUP) for h in range(n)]
            for c in range(4)
        ]
        outputs = [(1, sum(widths[h] for h in halves))] * GROUP
        return swap(gather(buffers, outputs, cases, AT_CASE + o))

    def add(o, windows, halves, total=None, part=None, kind=jnp.float32):
        windows = [tie(windows[0], last_step)] + windows[1:]
        return gain_group(
            table, AT_BLOCK + o * GROUP, windows, weights, halves[0] * widths[0], depth, shares, total, part, kind
        )

    share_at = table[AT_SHARE]
    shape = (STEPS, trials, share)
    came = []

    def send(part, k):
        arrived = lax.ppermute(part, "tgt", [(t, (t + k) % shares) for t in range(shares)])
        came.append(arrived.reshape(shape))

    outs = gather(
        turned, [(slot_count, widths[h]) for h in ab for _ in ab],
        [[(h, at_slot(f, k), 2 * h + f, k, 0) for h in ab for f in ab for k in range(slot_count)]],
    )
    for h in ab:
        for f, d in enumerate((1, -1)):
            slots[1, d, h] = hop(outs[2 * h + f], 1, d, True)
            full[1, d, h] = hop(turned[h], 1, d, False)
    own = gather(
        turned, [(1, piece)] * GROUP,
        [[(h, at_window(0, j), j, 0, h * widths[0]) for j in range(GROUP) for h in ab]],
    )
    own = swap(own)
    forward(2, 0)
    first = windows_of(1, ab)
    forward(2, 1)
    total = add(0, own, ab)
    second = [windows_of(2, (0,))]
    forward(3, 0)
    second += [windows_of(2, (1,))]
    send(add(1, first, ab, total, 1), 1)
    early = add(1, first, ab, total, 0)
    forward(3, 1)
    third = [windows_of(3, (0,))]
    late = add(2, second[0], (0,))
    third += [windows_of(3, (1,))]
    given = add(3, third[0], (0,), add(2, second[1], (1,), late, 1), 1)
    send(add(3, third[1], (1,), given, 1, jnp.bfloat16), 1)
    kept = add(3, third[0], (0,), add(2, second[1], (1,), late, 0), 0)
    kept = add(3, third[1], (1,), kept, 0)
    return advance(
        share_at, [], came + [early.reshape(shape), kept.reshape(shape)], potential, leak, drive
    )


def gather_all(history, weights, delays, boundary, potential, leak, drive, *, size, shares, spread):
    block_count, piece, targets = weights.shape
    trials = potential.shape[0]
    hist = history.shape[1] // trials
    per = trials // SUB
    depth = STEPS * trials
    chunks = max(1, min(CHUNKS, piece // 128))
    width = piece // chunks
    share = targets // shares
    blocks = jnp.arange(block_count, dtype=jnp.int32)
    area = jnp.sum((boundary[None, :] <= blocks[:, None]).astype(jnp.int32), axis=1)
    my_area = area[lax.axis_index("blk")]
    share_at = lax.axis_index("tgt")
    starts = ((hist - delays[my_area][area]) * per).astype(jnp.int32)

    turned = turn(history, [width] * chunks)
    arrived = [
        lax.all_gather(t, "blk", axis=0, tiled=False).reshape(size, hist * per, SUB, width) for t in turned
    ]
    own, came, total = [], [], None
    for c in range(chunks):
        if c < chunks - 2:
            (total,) = gain(starts, arrived[c], weights, c, depth, shares, total)
        elif c == chunks - 2:
            (early,) = gain(starts, arrived[c], weights, c, depth, shares, total, (jnp.float32,))
            own.append(early.reshape(shares, STEPS, trials, share))
            came += spread(early)
        else:
            late, late_low = gain(
                starts, arrived[c], weights, c, depth, shares, None, (jnp.float32, jnp.bfloat16 if chunks > 1 else jnp.float32)
            )
            own.append(late.reshape(shares, STEPS, trials, share))
            came += spread(late_low)
    return advance(share_at, own, came, potential, leak, drive)


def on_device(history, weights, delays, area_blocks, potential, leak, drive, *, size, shares):
    _, piece, targets = weights.shape
    trials = potential.shape[0]
    share = targets // shares
    boundary = jnp.cumsum(area_blocks)
    share_at = lax.axis_index("tgt")

    def spread(sums):
        came = []
        for k in range(1, shares):
            part = lax.dynamic_index_in_dim(sums, (share_at + k) % shares, 0, False)
            part = lax.ppermute(part, "tgt", [(t, (t + k) % shares) for t in range(shares)])
            came.append(part.reshape(STEPS, trials, share))
        return came

    if size != LINE * GROUP or shares != 2 or piece % 128 or piece < 256:
        return tuple(
            gather_all(history, weights, delays, boundary, potential, leak, drive, size=size, shares=shares, spread=spread)
        )
    me = lax.axis_index("blk")
    per = trials // SUB
    place = jnp.stack([me // GROUP, me % GROUP, share_at])
    table = plan(area_blocks, delays, place, history.shape[1] // trials, per)
    history = lax.optimization_barrier((history, table))[0]
    first_width = piece * 5 // 8 // 128 * 128
    turned = [t.reshape(-1, SUB, t.shape[1]) for t in turn(history, (first_width, piece - first_width))]
    line = functools.partial(line_of_groups, size=size, shares=shares)
    rest = (table, turned, weights, potential, leak, drive)
    if FORCE is not None:
        return tuple(line(FORCE, *rest))

    def branch(count):
        def run(*rest):
            return line(count, *rest)

        return run

    branches = [branch(count) for count in range(3, GROUP + 1)]
    return tuple(lax.switch(jnp.clip(table[AT_COUNT] - 2, 0, GROUP - 3), branches, *rest))


def solution(mesh):
    in_specs = (
        P(("blk", "tgt"), None),
        P(None, "tgt", "blk"),
        P(),
        P(),
        P(None, ("blk", "tgt")),
        P(("blk", "tgt")),
        P(("blk", "tgt")),
    )
    out_specs = (P(None, None, ("blk", "tgt")), P(None, ("blk", "tgt")))
    return jax.shard_map(
        functools.partial(on_device, size=mesh.shape["blk"], shares=mesh.shape["tgt"]),
        mesh=mesh, in_specs=in_specs, out_specs=out_specs, check_vma=False,
    )
```
